32 devices in a mesh: expert: 8 (over z, x), dp: 4 (over y, core).
Axes of the slice: x: 2, y: 2, z: 4, core: 2. Of those that a mesh axis runs over, the one named last changes fastest.
Arguments:
- tokens: bfloat16 [4096, 2048], P(('expert', 'dp')), may hold values from -6 to 6
- expert_ids: int32 [4096, 2], P(('expert', 'dp')), may hold values from 0 to 7, all different within a row; in each aligned block of 128 rows (0 to 127, 128 to 255, ...) at most 48 rows name the same one
- gate_scores: float32 [4096, 2], P(('expert', 'dp')), may hold values from 0.2 to 1
- gate_proj: bfloat16 [8, 768, 2048], P('expert', 'dp'), may hold values from -0.125 to 0.125
- up_proj: bfloat16 [8, 768, 2048], P('expert', 'dp'), may hold values from -0.125 to 0.125
- down_proj: bfloat16 [8, 768, 2048], P('expert', 'dp'), may hold values from -0.21875 to 0.21875
- out_grad: bfloat16 [4096, 2048], P(('expert', 'dp')), may hold values from -0.59765625 to 0.59765625
Outputs:
- output: bfloat16 [4096, 2048], P(('expert', 'dp'))
- d_tokens: bfloat16 [4096, 2048], P(('expert', 'dp'))
- d_scores: float32 [4096, 2], P(('expert', 'dp'))
- d_gate_proj: bfloat16 [8, 768, 2048], P('expert', 'dp')
- d_up_proj: bfloat16 [8, 768, 2048], P('expert', 'dp')
- d_down_proj: bfloat16 [8, 768, 2048], P('expert', 'dp')
The draws below stay inside these ranges and needn't reach their ends.
Inputs may be any that keep to these rules, and one draw needn't show every extreme that they name: `expert_ids`: each token names 2 different experts. Among the routes of one device's 128 tokens no expert is named more than 48 times, and in some devices' blocks some expert is named exactly 48 times.
All inputs are finite; a program needn't handle non-finite values.
Results may differ from the reference program's by a relative error of at most 0.014.
Values may be sent and summed in bfloat16 or wider, within the bound.
No kernel may reach another device: no remote copies, remote signals or barrier semaphores. Data moves between devices by JAX's collectives and lax.ppermute only.
A program may use at most 128 MiB of HBM per device.

```python
import math
import jax
import jax.numpy as jnp
import numpy as np
from jax import lax

D = 2048
FF = 768
TOP = 2
TOK_DEV = 128
EXPERTS = 8
CAP = 48
TOKENS = 4096
N_EXPERT = 8
N_DP = 4


def shard_levels(own_key, dims, shards, low, high):
    gain = 1.0
    for dim, parts in shards:
        heights = jax.random.uniform(jax.random.fold_in(jax.random.fold_in(own_key, 6), dim), (parts,), jnp.float32, low / len(shards), high / len(shards))
        gain = gain * jnp.repeat(jnp.exp(heights), dims[dim] // parts).reshape((-1,) + (1,) * (len(dims) - 1 - dim))
    return gain


def assign_block(stream_key, own, number, rows, number_of, top, limit, skew):
    order = jax.random.permutation(stream_key, number_of)
    packed, usual = shares(number_of, rows * top, limit, skew, True), shares(number_of, rows * top, limit, skew, False)
    places = jnp.arange(number_of)

    def named(lengths, turn):
        used = int((lengths > 0).sum())
        fixed = max(1, used // 4)
        moved = fixed + (places - fixed + turn * (used - fixed)) % max(1, number_of - fixed)
        return jnp.zeros((number_of,), jnp.int32).at[order[jnp.where(places < fixed, places, moved)]].set(jnp.asarray(lengths, jnp.int32))

    lengths = jnp.where(number % 4 == 0, named(packed, number // 4), named(usual, number - number // 4 - 1))
    mixed = jax.random.permutation(jax.random.fold_in(own, 3), number_of)
    source_of, sink = mixed[0:number_of // 2 * 2:2], mixed[1:number_of // 2 * 2:2]
    room = jnp.minimum(lengths[source_of] - 1, limit - lengths[sink]) // 2
    room = jnp.where((source_of == order[0]) | (sink == order[0]) | (lengths[sink] == 0), 0, jnp.maximum(room, 0))
    moved = jax.random.randint(jax.random.fold_in(own, 4), (number_of // 2,), 0, 1 << 20) % (room + 1)
    lengths = lengths.at[source_of].add(-moved).at[sink].add(moved)
    members = jnp.searchsorted(jnp.cumsum(lengths), jnp.arange(rows * top), side="right").astype(jnp.int32)
    listing = members.reshape(top, rows).T
    listing = listing[jax.random.permutation(jax.random.fold_in(own, 1), rows)]
    turn = jax.random.randint(jax.random.fold_in(own, 2), (rows, 1), 0, top)
    return jnp.take_along_axis(listing, (jnp.arange(top)[None, :] + turn) % top, axis=1)


def shares(count, total, limit, skew, full):
    weights = [(1 << 20) // math.isqrt(grade ** skew) + 1 for grade in range(1, count + 1)]
    largest = limit if full else min(limit, max(-(-total // count), total * weights[0] // sum(weights)))
    least = 1 if total - largest >= count - 1 else 0
    holding, rest = [largest] + [least] * (count - 1), total - largest - least * (count - 1)
    while rest > 0:
        candidates = [i for i in range(1, count) if holding[i] < largest] or [i for i in range(1, count) if holding[i] < limit]
        mass, budget = sum([weights[i] for i in candidates]), rest
        for i in candidates:
            more = min(limit - holding[i], max(1, budget * weights[i] // mass), rest)
            holding[i] = holding[i] + more
            rest = rest - more
    return np.array(holding)


def noise(key, shape, spread, most, split=(), held_as=jnp.bfloat16):
    result = spread * jax.random.normal(key, shape, jnp.float32)
    if split:
        result = result * shard_levels(key, shape, split, -0.22, 0.18)
    return jnp.clip(result, -most, most).astype(held_as)


def setup_inputs(seed: int = 0) -> dict:
    key_list = jax.random.split(jax.random.key(seed), 8)
    tokens = noise(key_list[0], (TOKENS, D), 1.0, 6.0, ((0, 32),))
    expert_ids_keys = jax.random.split(jax.random.fold_in(key_list[1], 1), TOKENS // TOK_DEV)
    expert_ids_turns = jax.random.permutation(jax.random.fold_in(key_list[1], 3), TOKENS // TOK_DEV)
    expert_ids = jax.vmap(lambda own, number: assign_block(jax.random.fold_in(key_list[1], 2), own, number, TOK_DEV, EXPERTS, TOP, CAP, 2))(expert_ids_keys, expert_ids_turns).reshape((TOKENS, TOP))
    gate_scores = jnp.clip(0.2 + 0.8 * jax.random.uniform(key_list[2], (TOKENS, TOP), jnp.float32) ** shard_levels(key_list[2], (TOKENS, TOP), ((0, 32),), -0.2, 0.2), 0.2, 1.0)
    gate_proj = noise(key_list[3], (EXPERTS, FF, D), D ** -0.5, 0.125, ((0, 8), (1, 4)))
    up_proj = noise(key_list[4], (EXPERTS, FF, D), D ** -0.5, 0.125, ((0, 8), (1, 4)))
    down_proj = noise(key_list[5], (EXPERTS, FF, D), FF ** -0.5, 0.21875, ((0, 8), (1, 4)))
    out_grad = noise(key_list[6], (TOKENS, D), 0.1, 0.59765625, ((0, 32),))
    return {"tokens": tokens, "expert_ids": expert_ids, "gate_scores": gate_scores, "gate_proj": gate_proj, "up_proj": up_proj, "down_proj": down_proj, "out_grad": out_grad}


def silu_parts(preact):
    logistic = jax.nn.sigmoid(preact)
    return preact * logistic, logistic * (1.0 + preact * (1.0 - logistic))


def regroup(values):
    shaped = values.reshape(N_EXPERT, N_DP, CAP, values.shape[-1])
    return jnp.transpose(shaped, (1, 0, 2, 3)).reshape(N_DP, N_EXPERT * CAP, values.shape[-1])


def per_group(left_rows, right_rows):
    left_rows = regroup(left_rows).astype(jnp.float32)
    right_rows = regroup(right_rows).astype(jnp.float32)
    partial_value = jnp.einsum("gsf,gsd->gfd", left_rows, right_rows)
    rounded = lax.optimization_barrier(partial_value.astype(jnp.bfloat16))
    return jnp.sum(rounded.astype(jnp.float32), axis=0).astype(jnp.bfloat16)


def reference(tokens, expert_ids, gate_scores, gate_proj, up_proj, down_proj, out_grad):
    devices = N_EXPERT * N_DP
    pair_total = TOKENS * TOP
    block_ids = expert_ids.reshape(devices, TOK_DEV * TOP)
    onehot = (block_ids[:, :, None] == jnp.arange(EXPERTS, dtype=jnp.int32)[None, None, :]).astype(jnp.int32)
    position = jnp.sum(jnp.cumsum(onehot, axis=1) * onehot, axis=2) - 1
    source = jnp.arange(devices, dtype=jnp.int32)[:, None]
    target = ((block_ids * devices + source) * CAP + position).reshape(-1).astype(jnp.int32)
    slot_table = jnp.full((EXPERTS * devices * CAP,), pair_total, dtype=jnp.int32)
    slot_table = slot_table.at[target].set(jnp.arange(pair_total, dtype=jnp.int32))
    padded_tokens = jnp.concatenate([tokens, jnp.zeros((1, D), tokens.dtype)], axis=0)
    padded_grad = jnp.concatenate([out_grad, jnp.zeros((1, D), out_grad.dtype)], axis=0)
    padded_scores = jnp.concatenate([gate_scores.reshape(-1), jnp.zeros((1,), jnp.float32)])

    def one_expert(operands):
        slot_ids, gate_w, up_w, down_w = operands
        token_ids = slot_ids // TOP
        gathered = padded_tokens[token_ids]
        gate_pre = jnp.dot(gathered, gate_w.T, preferred_element_type=jnp.float32)
        up_pre = jnp.dot(gathered, up_w.T, preferred_element_type=jnp.float32)
        activated, silu_slope = silu_parts(gate_pre)
        hidden = (activated * up_pre).astype(jnp.bfloat16)
        expert_out = jnp.dot(hidden, down_w, preferred_element_type=jnp.float32).astype(jnp.bfloat16)
        out_cot = (padded_scores[slot_ids][:, None] * padded_grad[token_ids].astype(jnp.float32)).astype(jnp.bfloat16)
        hidden_grad = jnp.dot(out_cot, down_w.T, preferred_element_type=jnp.float32)
        gate_grad = (hidden_grad * up_pre * silu_slope).astype(jnp.bfloat16)
        up_grad = (hidden_grad * activated).astype(jnp.bfloat16)
        input_grad = (jnp.dot(gate_grad, gate_w, preferred_element_type=jnp.float32)
                      + jnp.dot(up_grad, up_w, preferred_element_type=jnp.float32)).astype(jnp.bfloat16)
        return (expert_out, input_grad, per_group(gate_grad, gathered),
                per_group(up_grad, gathered), per_group(hidden, out_cot))

    expert_out, input_grad, d_gate_proj, d_up_proj, d_down_proj = lax.map(
        one_expert, (slot_table.reshape(EXPERTS, devices * CAP), gate_proj, up_proj, down_proj))
    flat_slots = slot_table.reshape(-1)
    pair_out = jnp.zeros((pair_total + 1, D), jnp.bfloat16).at[flat_slots].set(expert_out.reshape(-1, D))[:pair_total]
    pair_input = jnp.zeros((pair_total + 1, D), jnp.bfloat16).at[flat_slots].set(input_grad.reshape(-1, D))[:pair_total]
    pair_out = pair_out.reshape(TOKENS, TOP, D).astype(jnp.float32)
    output = jnp.sum(gate_scores[:, :, None] * pair_out, axis=1).astype(jnp.bfloat16)
    d_scores = jnp.sum(out_grad.astype(jnp.float32)[:, None, :] * pair_out, axis=2)
    d_tokens = jnp.sum(pair_input.reshape(TOKENS, TOP, D).astype(jnp.float32), axis=1).astype(jnp.bfloat16)
    return output, d_tokens, d_scores, d_gate_proj, d_up_proj, d_down_proj
```

```python
import functools

import jax
import jax.numpy as jnp
from jax import lax
from jax.experimental import pallas as pl
from jax.experimental.pallas import tpu as pltpu
from jax.sharding import PartitionSpec as P


F32 = jnp.float32
BF16 = jnp.bfloat16
VMEM = pl.BlockSpec(memory_space=pltpu.VMEM)
SMEM = pl.BlockSpec(memory_space=pltpu.SMEM)


def silu_parts(preact):
    logistic = jax.nn.sigmoid(preact)
    return (preact * logistic, logistic * (1.0 + preact * (1.0 - logistic)))


def col_tiles(width, step=512):
    step = min(width, step)
    return [slice(n, min(n + step, width)) for n in range(0, width, step)]


def slot_rows(ids_ref, me, experts, capacity):
    routes, toks = ids_ref.shape
    rows = lax.broadcasted_iota(jnp.int32, (experts, toks), 0)
    earlier = (
        lax.broadcasted_iota(jnp.int32, (toks, toks), 0)
        < lax.broadcasted_iota(jnp.int32, (toks, toks), 1)
    ).astype(BF16)
    base = jnp.zeros((experts, 1), F32)
    slots = []
    for k in range(routes):
        rel = ids_ref[k : k + 1, :] ^ me
        named = (rows == rel).astype(F32)
        before = jnp.dot(named.astype(BF16), earlier, preferred_element_type=F32) + base
        base = base + jnp.sum(named, axis=1, keepdims=True)
        place = jnp.sum(before * named, axis=0, keepdims=True)
        slots.append(rel * capacity + place.astype(jnp.int32))
    return slots


def pick(slot, slot_total):
    toks = slot.shape[1]
    return lax.broadcasted_iota(jnp.int32, (slot_total, toks), 0) == slot


def store_chunks(refs, cols, value):
    rows = refs[0].shape[0]
    for r, ref in enumerate(refs):
        ref[:, cols] = value[r * rows : (r + 1) * rows]


def send_tokens_kernel(experts, capacity, me_ref, ids_ref, tokens_ref, slots_ref, *chunk_refs):
    slots = slot_rows(ids_ref, me_ref[0], experts, capacity)
    chosen = None
    for k, slot in enumerate(slots):
        slots_ref[k : k + 1, :] = slot
        hit = pick(slot, experts * capacity)
        chosen = hit if chosen is None else chosen | hit
    chosen = chosen.astype(F32).astype(BF16)
    for cols in col_tiles(tokens_ref.shape[1]):
        rows = jnp.dot(chosen, tokens_ref[:, cols], preferred_element_type=F32)
        store_chunks(chunk_refs, cols, rows.astype(BF16))


def send_cots_kernel(experts, capacity, slots_ref, scores_ref, grad_ref, *chunk_refs):
    chosen, weight = None, None
    for k in range(slots_ref.shape[0]):
        hit = pick(slots_ref[k : k + 1, :], experts * capacity)
        scaled = jnp.where(hit, scores_ref[k : k + 1, :], 0.0)
        chosen = hit if chosen is None else chosen | hit
        weight = scaled if weight is None else weight + scaled
    weight = jnp.sum(weight, axis=1, keepdims=True)
    chosen = chosen.astype(F32).astype(BF16)
    for cols in col_tiles(grad_ref.shape[1]):
        rows = jnp.dot(chosen, grad_ref[:, cols], preferred_element_type=F32)
        store_chunks(chunk_refs, cols, (rows * weight).astype(BF16))


def gather_rows(hit, rows):
    return lax.dot_general(hit, rows, (((0,), (0,)), ((), ())), preferred_element_type=F32)


def dot_nt(left, right):
    return lax.dot_general(left, right, (((1,), (1,)), ((), ())), preferred_element_type=F32)


def load_rows(chunk_refs, rows_ref):
    rows = chunk_refs[0].shape[0]
    for r, ref in enumerate(chunk_refs):
        rows_ref[r * rows : (r + 1) * rows, :] = ref[...]


def load_chunks(refs, cols):
    return jnp.concatenate([ref[:, cols] for ref in refs], axis=0)


def combine_out_kernel(slot_total, slots_ref, scores_ref, grad_ref, *refs):
    *chunk_refs, out_ref, dscore_ref = refs
    routes = slots_ref.shape[0]
    hits = [pick(slots_ref[k : k + 1, :], slot_total).astype(F32).astype(BF16) for k in range(routes)]
    dots = [jnp.zeros((grad_ref.shape[0], 1), F32) for _ in range(routes)]
    for cols in col_tiles(grad_ref.shape[1]):
        rows = load_chunks(chunk_refs, cols)
        grad = grad_ref[:, cols].astype(F32)
        total = None
        for k in range(routes):
            pair = gather_rows(hits[k], rows)
            dots[k] = dots[k] + jnp.sum(pair * grad, axis=1, keepdims=True)
            term = scores_ref[:, k : k + 1] * pair
            total = term if total is None else total + term
        out_ref[:, cols] = total.astype(BF16)
    for k in range(routes):
        dscore_ref[:, k : k + 1] = dots[k]


def combine_grad_kernel(slot_total, slots_ref, *refs):
    *chunk_refs, out_ref = refs
    chosen = None
    for k in range(slots_ref.shape[0]):
        hit = pick(slots_ref[k : k + 1, :], slot_total)
        chosen = hit if chosen is None else chosen | hit
    chosen = chosen.astype(F32).astype(BF16)
    for cols in col_tiles(out_ref.shape[1]):
        out_ref[:, cols] = gather_rows(chosen, load_chunks(chunk_refs, cols)).astype(BF16)


def expert_in_kernel(gate_ref, up_ref, *refs):
    *chunk_refs, rows_ref, hidden_ref, act_ref, slope_ref = refs
    load_rows(chunk_refs, rows_ref)
    rows = rows_ref[...]
    for cols in col_tiles(hidden_ref.shape[1], 256):
        gate_pre = dot_nt(rows, gate_ref[cols, :])
        up_pre = dot_nt(rows, up_ref[cols, :])
        activated, slope = silu_parts(gate_pre)
        hidden_ref[:, cols] = (activated * up_pre).astype(BF16)
        act_ref[:, cols] = activated
        slope_ref[:, cols] = slope * up_pre


def expert_out_kernel(hidden_ref, down_ref, *chunk_refs):
    hidden = hidden_ref[...]
    for cols in col_tiles(down_ref.shape[1]):
        store_chunks(chunk_refs, cols, jnp.dot(hidden, down_ref[:, cols], preferred_element_type=F32).astype(BF16))


def hidden_grad_kernel(down_ref, act_ref, slope_ref, cots_ref, gate_grad_ref, up_grad_ref):
    cots = cots_ref[...]
    for cols in col_tiles(act_ref.shape[1], 256):
        hidden_grad = dot_nt(cots, down_ref[cols, :])
        gate_grad_ref[:, cols] = (hidden_grad * slope_ref[:, cols]).astype(BF16)
        up_grad_ref[:, cols] = (hidden_grad * act_ref[:, cols]).astype(BF16)


def input_grad_kernel(gate_grad_ref, up_grad_ref, gate_ref, up_ref, *chunk_refs):
    gate_grad, up_grad = gate_grad_ref[...], up_grad_ref[...]
    for cols in col_tiles(gate_ref.shape[1]):
        total = jnp.dot(gate_grad, gate_ref[:, cols], preferred_element_type=F32)
        total = total + jnp.dot(up_grad, up_ref[:, cols], preferred_element_type=F32)
        store_chunks(chunk_refs, cols, total.astype(BF16))


def weight_grad_kernel(left_ref, right_ref, *part_refs):
    step = part_refs[0].shape[0]
    per = 2 if len(part_refs) % 2 == 0 else len(part_refs)
    for first in range(0, len(part_refs), per):
        left = left_ref[:, first * step : (first + per) * step]
        for cols in col_tiles(right_ref.shape[1]):
            store_chunks(part_refs[first : first + per], cols, gather_rows(left, right_ref[:, cols]).astype(BF16))


def join_kernel(*refs):
    *chunk_refs, rows_ref = refs
    load_rows(chunk_refs, rows_ref)


def add_kernel(*refs):
    *term_refs, out_ref = refs
    total = term_refs[0][...].astype(F32)
    for ref in term_refs[1:]:
        total = total + ref[...].astype(F32)
    out_ref[...] = total.astype(BF16)


def add(terms):
    return call(add_kernel, terms, jax.ShapeDtypeStruct(terms[0].shape, BF16))


def call(kernel, args, shapes, flops=0):
    single = not isinstance(shapes, list)
    return pl.pallas_call(
        kernel,
        out_shape=shapes,
        in_specs=[SMEM if a.ndim == 1 else VMEM for a in args],
        out_specs=VMEM if single else [VMEM] * len(shapes),
        cost_estimate=pl.CostEstimate(flops=flops, transcendentals=0, bytes_accessed=0),
        compiler_params=pltpu.CompilerParams(vmem_limit_bytes=24 * 1024 * 1024),
    )(*args)


def swap(value, axis, size, bits):
    return lax.ppermute(value, axis, [(i, i ^ bits) for i in range(size)])


def exchange(chunks, size):
    if len(chunks) == 1:
        rows, width = chunks[0].shape
        moved = lax.all_to_all(
            chunks[0].reshape(size, rows // size, width), "expert", split_axis=0, concat_axis=0, tiled=True
        )
        return [moved.reshape(rows, width)]
    got = {0: chunks[0]}
    for j in sorted(range(1, size), reverse=True):
        got[j] = swap(chunks[j], "expert", size, j)
    return [got[j] for j in range(size)]


def gather_shards(shard, size):
    have = {0: shard}
    bit = size // 2
    while bit:
        for j in list(have):
            have[j ^ bit] = swap(have[j], "dp", size, bit)
        bit //= 2
    return call(join_kernel, [have[j] for j in range(size)], jax.ShapeDtypeStruct((size * shard.shape[0], shard.shape[1]), BF16))


def scatter_sum(parts, size):
    terms = {j: [part] for j, part in enumerate(parts)}
    bit = 1
    while bit < size:
        for j in sorted((j for j in terms if j & bit), reverse=True):
            sent = terms.pop(j)
            sent = sent[0] if len(sent) == 1 else add(sent)
            terms[j ^ bit].append(swap(sent, "dp", size, bit))
        bit *= 2
    return add(terms[0])


def body(tokens, expert_ids, gate_scores, gate_proj, up_proj, down_proj, out_grad):
    tok_count, width = tokens.shape
    routes = expert_ids.shape[1]
    experts = lax.axis_size("expert")
    n_dp = lax.axis_size("dp")
    capacity = max(2, 3 * tok_count * routes // (2 * experts))
    slot_total = experts * capacity
    chunked = experts & (experts - 1) == 0 and experts <= 8 and capacity % 16 == 0
    n_chunks = experts if chunked else 1
    units = gate_proj.shape[1] * n_dp
    flops = 2 * slot_total * width * units

    def shape(rows, cols, dtype=BF16):
        return jax.ShapeDtypeStruct((rows, cols), dtype)

    chunk_shapes = [shape(slot_total // n_chunks, width)] * n_chunks
    part_shapes = [shape(units // n_dp, width)] * n_dp

    gate_w = gather_shards(gate_proj[0], n_dp)
    up_w = gather_shards(up_proj[0], n_dp)
    down_w = gather_shards(down_proj[0], n_dp)

    me = (lax.axis_index("expert") if chunked else jnp.int32(0)).astype(jnp.int32).reshape(1)
    slots, *token_chunks = call(
        functools.partial(send_tokens_kernel, experts, capacity),
        [me, expert_ids.T, tokens],
        [shape(routes, tok_count, jnp.int32)] + chunk_shapes,
        flops // 10,
    )
    token_chunks = exchange(token_chunks, experts)
    cot_chunks = call(
        functools.partial(send_cots_kernel, experts, capacity),
        [slots, gate_scores.T, out_grad],
        chunk_shapes,
        flops // 10,
    )
    cot_chunks = exchange(cot_chunks, experts)

    received, hidden, act, slope = call(
        expert_in_kernel,
        [gate_w, up_w, *token_chunks],
        [shape(slot_total, width), shape(slot_total, units), shape(slot_total, units, F32), shape(slot_total, units, F32)],
        2 * flops,
    )
    out_chunks = call(expert_out_kernel, [hidden, down_w], chunk_shapes, flops)
    out_back = exchange(out_chunks, experts)

    cot_rows = call(join_kernel, cot_chunks, shape(slot_total, width))
    down_parts = call(weight_grad_kernel, [hidden, cot_rows], part_shapes, flops)
    gate_grad, up_grad = call(hidden_grad_kernel, [down_w, act, slope, cot_rows], [shape(slot_total, units)] * 2, flops)
    gate_parts = call(weight_grad_kernel, [gate_grad, received], part_shapes, flops)
    up_parts = call(weight_grad_kernel, [up_grad, received], part_shapes, flops)
    grad_chunks = call(input_grad_kernel, [gate_grad, up_grad, gate_w, up_w], chunk_shapes, 2 * flops)
    grad_back = exchange(grad_chunks, experts)

    down_out = scatter_sum(down_parts, n_dp)[None]
    gate_out = scatter_sum(gate_parts, n_dp)[None]
    up_out = scatter_sum(up_parts, n_dp)[None]

    output, d_scores = call(
        functools.partial(combine_out_kernel, slot_total),
        [slots, gate_scores, out_grad, *out_back],
        [shape(tok_count, width), shape(tok_count, routes, F32)],
        flops // 5,
    )
    d_tokens = call(
        functools.partial(combine_grad_kernel, slot_total), [slots, *grad_back], shape(tok_count, width), flops // 10
    )
    return (output, d_tokens, d_scores, gate_out, up_out, down_out)


def solution(mesh):
    rows = P(("expert", "dp"), None)
    weights = P("expert", "dp", None)
    return jax.shard_map(
        body,
        mesh=mesh,
        in_specs=(rows, rows, rows, weights, weights, weights, rows),
        out_specs=(rows, rows, rows, weights, weights, weights),
        check_vma=False,
    )
```

```python
import functools

import jax
import jax.numpy as jnp
from jax import lax
from jax.experimental import pallas as pl
from jax.experimental.pallas import tpu as pltpu
from jax.sharding import PartitionSpec as P


EX, DP = "expert", "dp"
F32 = jnp.float32
BF16 = jnp.bfloat16
VMEM = pl.BlockSpec(memory_space=pltpu.VMEM)
SMEM = pl.BlockSpec(memory_space=pltpu.SMEM)
GRANT = 24 * 1024 * 1024


def silu_parts(preact):
    logistic = jax.nn.sigmoid(preact)
    return (preact * logistic, logistic * (1.0 + preact * (1.0 - logistic)))


def col_tiles(width, step=512):
    step = min(width, step)
    return [slice(n, min(n + step, width)) for n in range(0, width, step)]


def dot_nt(left, right):
    return lax.dot_general(left, right, (((1,), (1,)), ((), ())), preferred_element_type=F32)


def dot_tn(left, right):
    return lax.dot_general(left, right, (((0,), (0,)), ((), ())), preferred_element_type=F32)


def store_chunks(refs, cols, value):
    rows = refs[0].shape[0]
    for r, ref in enumerate(refs):
        ref[:, cols] = value[r * rows : (r + 1) * rows]


def window(ref, part):
    rows = ref.shape[0] if part is None else ref.shape[0] // 2
    return slice(part * rows if part else 0, (part or 0) * rows + rows)


def load_chunks(refs, cols, part=None):
    return jnp.concatenate([ref[window(ref, part), cols] for ref in refs], axis=0)


def load_rows(chunk_refs, rows_ref, part=None, first=0):
    for ref in chunk_refs:
        value = ref[window(ref, part), :]
        rows_ref[first : first + value.shape[0], :] = value
        first += value.shape[0]
    return first


def slots_kernel(experts, capacity, me_ref, ctl_ref, slots_ref):
    routes, toks = slots_ref.shape
    half = experts // 2
    rows = lax.broadcasted_iota(jnp.int32, (experts, toks), 0)
    earlier = (
        lax.broadcasted_iota(jnp.int32, (toks, toks), 0)
        < lax.broadcasted_iota(jnp.int32, (toks, toks), 1)
    ).astype(BF16)
    base = jnp.zeros((experts, 1), F32)
    for k in range(routes):
        rel = ctl_ref[k : k + 1, :].astype(jnp.int32) ^ me_ref[0]
        named = (rows == rel).astype(F32)
        before = jnp.dot(named.astype(BF16), earlier, preferred_element_type=F32) + base
        base = base + jnp.sum(named, axis=1, keepdims=True)
        rank = jnp.sum(before * named, axis=0, keepdims=True).astype(jnp.int32)
        slots_ref[k : k + 1, :] = jnp.where(rel < half, rel * capacity + rank, -1)


def pick(slot, slot_total):
    return lax.broadcasted_iota(jnp.int32, (slot_total, slot.shape[1]), 0) == slot


def as_bf16(hit):
    return hit.astype(F32).astype(BF16)


def as_column(row):
    toks = row.shape[1]
    same = lax.broadcasted_iota(jnp.int32, (toks, toks), 0) == lax.broadcasted_iota(jnp.int32, (toks, toks), 1)
    return jnp.sum(jnp.where(same, row, 0.0), axis=1, keepdims=True)


def as_row(column):
    toks = column.shape[0]
    same = lax.broadcasted_iota(jnp.int32, (toks, toks), 0) == lax.broadcasted_iota(jnp.int32, (toks, toks), 1)
    return jnp.sum(jnp.where(same, column, 0.0), axis=0, keepdims=True)


def chosen_rows(slots_ref, slot_total):
    chosen = None
    for k in range(slots_ref.shape[0]):
        hit = pick(slots_ref[k : k + 1, :], slot_total)
        chosen = hit if chosen is None else chosen | hit
    return as_bf16(chosen)


def send_tokens_kernel(slot_total, slots_ref, tokens_ref, *chunk_refs):
    chosen = chosen_rows(slots_ref, slot_total)
    for cols in col_tiles(tokens_ref.shape[1]):
        rows = jnp.dot(chosen, tokens_ref[:, cols], preferred_element_type=F32)
        store_chunks(chunk_refs, cols, rows.astype(BF16))


def slot_scores(slots_ref, ctl_ref, slot_total):
    routes = slots_ref.shape[0]
    weight = None
    for k in range(routes):
        hit = pick(slots_ref[k : k + 1, :], slot_total)
        score = jnp.where(hit, ctl_ref[routes + k : routes + k + 1, :], 0.0)
        weight = score if weight is None else weight + score
    return jnp.sum(weight, axis=1, keepdims=True)


def send_cots_kernel(slot_total, slots_ref, ctl_ref, grad_ref, *chunk_refs):
    weight = slot_scores(slots_ref, ctl_ref, slot_total)
    chosen = chosen_rows(slots_ref, slot_total)
    for cols in col_tiles(grad_ref.shape[1]):
        rows = jnp.dot(chosen, grad_ref[:, cols], preferred_element_type=F32)
        store_chunks(chunk_refs, cols, (rows * weight).astype(BF16))


def combine_out_kernel(slot_total, n_chunks, part, slots_ref, ctl_ref, grad_ref, *refs):
    chunk_refs, refs = refs[:n_chunks], refs[n_chunks:]
    *came_refs, out_ref, dscore_ref = refs
    routes = slots_ref.shape[0]
    hits, scores = [], []
    for k in range(routes):
        hits.append(as_bf16(pick(slots_ref[k : k + 1, :], slot_total)))
        scores.append(as_column(ctl_ref[routes + k : routes + k + 1, :]))
    dots = [jnp.zeros((grad_ref.shape[0], 1), F32) for _ in range(routes)]
    for cols in col_tiles(grad_ref.shape[1]):
        rows = load_chunks(chunk_refs, cols, part)
        grad = grad_ref[:, cols].astype(F32)
        total = came_refs[0][:, cols].astype(F32) if came_refs else None
        for k in range(routes):
            each = dot_tn(hits[k], rows)
            dots[k] = dots[k] + jnp.sum(each * grad, axis=1, keepdims=True)
            term = scores[k] * each
            total = term if total is None else total + term
        out_ref[:, cols] = total.astype(BF16)
    for k in range(routes):
        dscore = as_row(dots[k])
        if came_refs:
            dscore = dscore + came_refs[1][k : k + 1, :]
        dscore_ref[k : k + 1, :] = dscore


def combine_grad_kernel(slot_total, n_chunks, part, slots_ref, *refs):
    chunk_refs, refs = refs[:n_chunks], refs[n_chunks:]
    *came_refs, out_ref = refs
    chosen = chosen_rows(slots_ref, slot_total)
    for cols in col_tiles(out_ref.shape[1]):
        total = dot_tn(chosen, load_chunks(chunk_refs, cols, part))
        if came_refs:
            total = total + came_refs[0][:, cols].astype(F32)
        out_ref[:, cols] = total.astype(BF16)


def last_kernel(slot_total, n_chunks, first, second, slots_ref, ctl_ref, grad_ref, *refs):
    *refs, out_ref, dscore_ref, token_ref, up_ref = refs
    out_refs, refs = refs[:n_chunks], refs[n_chunks:]
    in_refs = out_refs
    if second is None:
        in_refs, refs = refs[:n_chunks], refs[n_chunks:]
    out_came_ref, dscore_came_ref, grad_came_ref, *up_refs = refs
    add_kernel(*up_refs, up_ref)
    combine_grad_kernel(slot_total, n_chunks, second, slots_ref, *in_refs, grad_came_ref, token_ref)
    combine_out_kernel(
        slot_total, n_chunks, first, slots_ref, ctl_ref, grad_ref, *out_refs, out_came_ref, dscore_came_ref, out_ref, dscore_ref
    )


def expert_in_kernel(n_shards, n_chunks, part, *refs):
    gate_refs, up_refs, refs = refs[:n_shards], refs[n_shards : 2 * n_shards], refs[2 * n_shards :]
    *chunk_refs, gate_ref, up_ref, rows_ref, hidden_ref, act_ref, slope_ref = refs
    load_rows(chunk_refs[n_chunks:], rows_ref, first=load_rows(chunk_refs[:n_chunks], rows_ref, part))
    load_rows(gate_refs, gate_ref)
    load_rows(up_refs, up_ref)
    rows = rows_ref[...]
    for cols in col_tiles(hidden_ref.shape[1], 256):
        gate_pre = dot_nt(rows, gate_ref[cols, :])
        up_pre = dot_nt(rows, up_ref[cols, :])
        activated, slope = silu_parts(gate_pre)
        hidden_ref[:, cols] = (activated * up_pre).astype(BF16)
        act_ref[:, cols] = activated
        slope_ref[:, cols] = slope * up_pre


def expert_out_kernel(n_shards, hidden_ref, *refs):
    shard_refs, down_ref, chunk_refs = refs[:n_shards], refs[n_shards], refs[n_shards + 1 :]
    load_rows(shard_refs, down_ref)
    hidden = hidden_ref[...]
    for cols in col_tiles(down_ref.shape[1]):
        store_chunks(chunk_refs, cols, jnp.dot(hidden, down_ref[:, cols], preferred_element_type=F32).astype(BF16))


def hidden_grad_kernel(down_ref, act_ref, slope_ref, cots_ref, gate_grad_ref, up_grad_ref):
    cots = cots_ref[...]
    for cols in col_tiles(act_ref.shape[1], 256):
        hidden_grad = dot_nt(cots, down_ref[cols, :])
        gate_grad_ref[:, cols] = (hidden_grad * slope_ref[:, cols]).astype(BF16)
        up_grad_ref[:, cols] = (hidden_grad * act_ref[:, cols]).astype(BF16)


def input_grad_kernel(n_chunks, gate_grad_ref, up_grad_ref, gate_ref, up_ref, *refs):
    out_refs, both_refs, pair_refs = refs[: -2 * n_chunks], refs[-2 * n_chunks : -n_chunks], refs[-n_chunks:]
    for out_ref, both_ref in zip(out_refs, both_refs):
        both_ref[window(both_ref, 0), :] = out_ref[...]
    part = 1 if out_refs else None
    gate_grad, up_grad = gate_grad_ref[...], up_grad_ref[...]
    for cols in col_tiles(gate_ref.shape[1]):
        total = jnp.dot(gate_grad, gate_ref[:, cols], preferred_element_type=F32)
        total = total + jnp.dot(up_grad, up_ref[:, cols], preferred_element_type=F32)
        total = total.astype(BF16)
        first = 0
        for ref, where in [(ref, window(ref, part)) for ref in both_refs] + [(ref, window(ref, None)) for ref in pair_refs]:
            count = where.stop - where.start
            ref[where, cols] = total[first : first + count]
            first += count


def weight_grad_kernel(left_ref, right_ref, *part_refs):
    step = part_refs[0].shape[0]
    per = 2 if len(part_refs) % 2 == 0 else len(part_refs)
    for first in range(0, len(part_refs), per):
        left = left_ref[:, first * step : (first + per) * step]
        for cols in col_tiles(right_ref.shape[1]):
            store_chunks(part_refs[first : first + per], cols, dot_tn(left, right_ref[:, cols]).astype(BF16))


def down_grad_kernel(n_chunks, part, hidden_ref, *refs):
    chunk_refs, rows_ref, part_refs = refs[: 2 * n_chunks], refs[2 * n_chunks], refs[2 * n_chunks + 1 :]
    load_rows(chunk_refs[n_chunks:], rows_ref, first=load_rows(chunk_refs[:n_chunks], rows_ref, part))
    weight_grad_kernel(hidden_ref, rows_ref, *part_refs)


def add_kernel(*refs):
    *term_refs, out_ref = refs
    total = term_refs[0][...].astype(F32)
    for ref in term_refs[1:]:
        total = total + ref[...].astype(F32)
    out_ref[...] = total.astype(BF16)


def call(kernel, args, shapes, flops=0):
    single = not isinstance(shapes, list)
    return pl.pallas_call(
        kernel,
        out_shape=shapes,
        in_specs=[SMEM if a.ndim == 1 else VMEM for a in args],
        out_specs=VMEM if single else [VMEM] * len(shapes),
        cost_estimate=pl.CostEstimate(flops=flops, transcendentals=0, bytes_accessed=0),
        compiler_params=pltpu.CompilerParams(vmem_limit_bytes=GRANT),
    )(*args)


def add(terms):
    return call(add_kernel, terms, jax.ShapeDtypeStruct(terms[0].shape, BF16))


def swap(value, axis, bits):
    return lax.ppermute(value, axis, [(i, i ^ bits) for i in range(lax.axis_size(axis))])


def pair_swap(value):
    return swap(value, EX, lax.axis_size(EX) // 2)


def exchange(chunks):
    size = lax.axis_size(EX)
    half = size // 2
    if len(chunks) == 1:
        rows, width = chunks[0].shape
        moved = lax.all_to_all(
            chunks[0].reshape(half, rows // half, width),
            EX,
            split_axis=0,
            concat_axis=0,
            tiled=True,
            axis_index_groups=[list(range(half)), list(range(half, size))],
        )
        return [moved.reshape(rows, width)]
    got = {0: chunks[0]}
    for j in range(half - 1, 0, -1):
        got[j] = swap(chunks[j], EX, j)
    return [got[j] for j in range(half)]


def gather_shards(shard):
    have = {0: shard}
    size = lax.axis_size(DP)
    bit = size // 2
    while bit:
        for j in list(have):
            have[j ^ bit] = swap(have[j], DP, bit)
        bit //= 2
    return [have[j] for j in range(size)]


def scatter_terms(parts):
    terms = {j: [part] for j, part in enumerate(parts)}
    bit = 1
    while bit < len(parts):
        for j in sorted((j for j in terms if j & bit), reverse=True):
            sent = terms.pop(j)
            sent = sent[0] if len(sent) == 1 else add(sent)
            terms[j ^ bit].append(swap(sent, DP, bit))
        bit *= 2
    return terms[0]


def body(tokens, expert_ids, gate_scores, gate_proj, up_proj, down_proj, out_grad):
    tok_count, width = tokens.shape
    routes = expert_ids.shape[1]
    experts = lax.axis_size(EX)
    n_dp = lax.axis_size(DP)
    half = experts // 2
    capacity = max(2, 3 * tok_count * routes // (2 * experts))
    slot_total = half * capacity
    chunked = experts == 8 and capacity % 16 == 0
    n_chunks = half if chunked else 1
    units = gate_proj.shape[1] * n_dp
    flops = 4 * slot_total * width * units

    def shape(rows, cols, dtype=BF16):
        return jax.ShapeDtypeStruct((rows, cols), dtype)

    chunk_shapes = [shape(slot_total // n_chunks, width)] * n_chunks
    both_shapes = [shape(2 * slot_total // n_chunks, width)] * n_chunks
    part_shapes = [shape(units // n_dp, width)] * n_dp
    act_shapes = [shape(2 * slot_total, units)] * 2

    own_ctl = jnp.concatenate([expert_ids.T.astype(F32), gate_scores.T], axis=0)
    pair_ctl = pair_swap(own_ctl)
    pair_tokens = pair_swap(tokens)
    pair_grad = pair_swap(out_grad)
    gate_s = gather_shards(gate_proj[0])
    up_s = gather_shards(up_proj[0])
    down_s = gather_shards(down_proj[0])

    me = lax.axis_index(EX).astype(jnp.int32).reshape(1)
    if not chunked:
        me = me // half * half

    def slots_of(ctl):
        kernel = functools.partial(slots_kernel, experts, capacity)
        return call(kernel, [me, ctl], shape(routes, tok_count, jnp.int32), flops // 100)

    def send_tokens(slots, rows):
        kernel = functools.partial(send_tokens_kernel, slot_total)
        sent = call(kernel, [slots, rows], chunk_shapes, flops // 20)
        return exchange(sent)

    def send_cots(slots, ctl, grad):
        kernel = functools.partial(send_cots_kernel, slot_total)
        sent = call(kernel, [slots, ctl, grad], chunk_shapes, flops // 20)
        return exchange(sent)

    own_slots = slots_of(own_ctl)
    own_tok = send_tokens(own_slots, tokens)
    own_cot = send_cots(own_slots, own_ctl, out_grad)
    pair_slots = slots_of(pair_ctl)
    pair_tok = send_tokens(pair_slots, pair_tokens)
    pair_cot = send_cots(pair_slots, pair_ctl, pair_grad)

    gate_w, up_w, received, hidden, act, slope = call(
        functools.partial(expert_in_kernel, n_dp, n_chunks, None),
        [*gate_s, *up_s, *own_tok, *pair_tok],
        [
            shape(units, width),
            shape(units, width),
            shape(2 * slot_total, width),
            shape(2 * slot_total, units),
            shape(2 * slot_total, units, F32),
            shape(2 * slot_total, units, F32),
        ],
        2 * flops,
    )
    cot_rows, *down_parts = call(
        functools.partial(down_grad_kernel, n_chunks, None),
        [hidden, *own_cot, *pair_cot],
        [shape(2 * slot_total, width)] + part_shapes,
        flops,
    )
    down_w, *out_chunks = call(
        functools.partial(expert_out_kernel, n_dp), [hidden, *down_s], [shape(units, width)] + 2 * chunk_shapes, flops
    )
    pair_out = exchange(out_chunks[n_chunks:])

    def combine_out(part, slots, ctl, grad, *rows):
        return call(
            functools.partial(combine_out_kernel, slot_total, n_chunks, part),
            [slots, ctl, grad, *rows],
            [shape(tok_count, width), shape(routes, tok_count, F32)],
            flops // 10,
        )

    out_part, dscore_part = combine_out(None, pair_slots, pair_ctl, pair_grad, *pair_out)
    out_came = pair_swap(out_part)
    dscore_came = pair_swap(dscore_part)

    gate_grad, up_grad = call(hidden_grad_kernel, [down_w, act, slope, cot_rows], act_shapes, flops)
    gate_parts = call(weight_grad_kernel, [gate_grad, received], part_shapes, flops)
    up_parts = call(weight_grad_kernel, [up_grad, received], part_shapes, flops)
    grad_chunks = call(
        functools.partial(input_grad_kernel, n_chunks),
        [gate_grad, up_grad, gate_w, up_w, *(out_chunks[:n_chunks] if chunked else [])],
        (both_shapes if chunked else chunk_shapes) + chunk_shapes,
        2 * flops,
    )
    own_grad = exchange(grad_chunks[:n_chunks])
    first, second = (0, 1) if chunked else (None, None)
    own_out = own_grad if chunked else exchange(out_chunks[:n_chunks])
    pair_in = exchange(grad_chunks[n_chunks:])

    def combine_grad(part, slots, *rows):
        return call(
            functools.partial(combine_grad_kernel, slot_total, n_chunks, part),
            [slots, *rows],
            shape(tok_count, width),
            flops // 20,
        )

    grad_came = pair_swap(combine_grad(None, pair_slots, *pair_in))

    down_out = add(scatter_terms(down_parts))[None]
    gate_out = add(scatter_terms(gate_parts))[None]
    up_terms = scatter_terms(up_parts)

    own_outs = [shape(tok_count, width), shape(routes, tok_count, F32), shape(tok_count, width), up_terms[0]]
    output, d_scores, d_tokens, up_out = call(
        functools.partial(last_kernel, slot_total, n_chunks, first, second),
        [own_slots, own_ctl, out_grad, *own_out, *(() if chunked else own_grad), out_came, dscore_came, grad_came, *up_terms],
        [jax.ShapeDtypeStruct(a.shape, a.dtype) for a in own_outs],
        flops // 5,
    )
    return (output, d_tokens, d_scores.T, gate_out, up_out[None], down_out)


def solution(mesh):
    rows = P((EX, DP), None)
    weights = P(EX, DP, None)
    return jax.shard_map(
        body,
        mesh=mesh,
        in_specs=(rows, rows, rows, weights, weights, weights, rows),
        out_specs=(rows, rows, rows, weights, weights, weights),
        check_vma=False,
    )
```
